32 devices in a mesh: img: 8 (over z, x), tile: 4 (over y, core).
Axes of the slice: x: 2, y: 2, z: 4, core: 2. Of those that a mesh axis runs over, the one named last changes fastest.
Arguments:
- query: bfloat16 [8, 512, 1280], P('img', 'tile'), may hold values from -6 to 6
- keys: bfloat16 [8, 512, 1280], P('img', 'tile'), may hold values from -6 to 6
- values: bfloat16 [8, 512, 1280], P('img', 'tile'), may hold values from -6 to 6
- out_weight: bfloat16 [1280, 1280], P('tile'), may hold values from -0.15625 to 0.15625
- hidden: bfloat16 [8, 512, 1280], P('img', 'tile'), may hold values from -36 to 36
- gain: float32 [1280], replicated, may hold values from 0.5 to 1.5
- seq_grad: bfloat16 [8, 512, 5120], P('img', 'tile'), may hold values from -6 to 6
- splice_at: int32 [8, 128], P('img', 'tile'), may hold values from 0 to 511, as said below
- merged_count: int32 [8], P('img'), may hold values from 16 to 128
Outputs:
- query_grad: bfloat16 [8, 512, 1280], P('img', 'tile')
- key_grad: bfloat16 [8, 512, 1280], P('img', 'tile')
- value_grad: bfloat16 [8, 512, 1280], P('img', 'tile')
- gain_grad: float32 [1280], replicated
The draws below stay inside these ranges and needn't reach their ends.
Inputs may be any that keep to these rules, and one draw needn't show every extreme that they name: `splice_at`: within one image the positions are distinct. The merged rows of one device (aligned blocks of 32 rows) place at most 16 rows in any one block of 128 positions of the sequence.
All inputs are finite; a program needn't handle non-finite values.
Results may differ from the reference program's by a relative error of at most 0.009.
Values may be sent and summed in bfloat16 or wider, within the bound.
No kernel may reach another device: no remote copies, remote signals or barrier semaphores. Data moves between devices by JAX's collectives and lax.ppermute only.
A program may use at most 64 MiB of HBM per device.

```python
import jax
import jax.numpy as jnp
from jax import lax

HEADS = 16
HEAD = 80
D = 1280
CTX_DEV = 128
IMAGES = 8
PATCHES = 512
MERGED = 128
MERGED_DEV = 32
CAP = 16
SEQ_LEN = 512


def drawn_pair(key):
    first = jax.random.fold_in(key, 11)
    second = jax.random.fold_in(key, 12)
    query_base = 1.5 * jax.random.truncated_normal(first, -4.0, 4.0, (IMAGES, PATCHES, D), jnp.float32)
    keys_base = 1.5 * jax.random.truncated_normal(second, -4.0, 4.0, (IMAGES, PATCHES, D), jnp.float32)
    return (query_base, keys_base)


def draw_query(key, part):
    return drawn_pair(key)[0].astype(jnp.bfloat16)


def draw_keys(key, part):
    return drawn_pair(key)[1].astype(jnp.bfloat16)


def draw_hidden(key, part):
    base_key = jax.random.fold_in(key, 21)
    row_key = jax.random.fold_in(key, 22)
    column_key = jax.random.fold_in(key, 23)
    base = jax.random.truncated_normal(base_key, -4.0, 4.0, (IMAGES, PATCHES, D), jnp.float32)
    row_scale = jnp.exp(jax.random.uniform(row_key, (IMAGES, PATCHES, 1), jnp.float32, jnp.log(0.3), jnp.log(3.0)))
    column_scale = jnp.exp(jax.random.uniform(column_key, (D,), jnp.float32, jnp.log(0.5), jnp.log(2.0)))
    return (base * row_scale * column_scale).astype(jnp.bfloat16)


def draw_splice_at(key, part):
    groups = MERGED // MERGED_DEV
    slot_total = groups * CAP
    full_key = jax.random.fold_in(key, 31)
    order_key = jax.random.fold_in(key, 32)
    shuffle_key = jax.random.fold_in(key, 33)
    place_key = jax.random.fold_in(key, 34)
    full_span = jax.random.randint(full_key, (IMAGES, 1, 1), 0, groups)
    order_keys = jax.random.split(order_key, IMAGES * groups)
    ranking = jax.vmap(lambda each: jax.random.permutation(each, slot_total))(order_keys).reshape(IMAGES, groups, slot_total)
    slot_range = jnp.arange(slot_total, dtype=jnp.int32)
    priority = ranking + jnp.where(slot_range // CAP == full_span, slot_total, 0)
    chosen = jnp.argsort(-priority, axis=-1, stable=True)[..., :MERGED_DEV]
    shuffle_keys = jax.random.split(shuffle_key, IMAGES * groups)
    shuffled = jax.vmap(lambda each: jax.random.permutation(each, MERGED_DEV))(shuffle_keys).reshape(IMAGES, groups, MERGED_DEV)
    chosen = jnp.take_along_axis(chosen, shuffled, axis=-1)
    spans = chosen // CAP
    within = chosen % CAP
    place_keys = jax.random.split(place_key, IMAGES * groups)
    places = jax.vmap(lambda each: jax.random.permutation(each, CTX_DEV))(place_keys).reshape(IMAGES, groups * CTX_DEV)
    sources = jnp.arange(groups, dtype=jnp.int32)[None, :, None]
    lookup = (spans * CTX_DEV + sources * CAP + within).reshape(IMAGES, MERGED)
    inside = jnp.take_along_axis(places, lookup, axis=1)
    return (spans.reshape(IMAGES, MERGED) * CTX_DEV + inside).astype(jnp.int32)


def place_ends(values, stream_key, least, high):
    index_at = [jax.random.randint(jax.random.fold_in(stream_key, axis), (), 0, length) for axis, length in enumerate(values.shape)]
    longest = values.shape.index(max(values.shape))
    beside = index_at[:longest] + [(index_at[longest] + 1) % values.shape[longest]] + index_at[longest + 1:]
    return values.at[tuple(index_at)].set(least).at[tuple(beside)].set(high)


def levels(own_key, shape, cuts, low, high):
    level = 1.0
    for axis_at, parts in cuts:
        steps = jax.random.uniform(jax.random.fold_in(jax.random.fold_in(own_key, 6), axis_at), (parts,), jnp.float32, low / len(cuts), high / len(cuts))
        level = level * jnp.repeat(jnp.exp(steps), shape[axis_at] // parts).reshape((-1,) + (1,) * (len(shape) - 1 - axis_at))
    return level


def bell_draw(own_key, shape, deviation, most, shards=(), kind=jnp.bfloat16):
    result = deviation * jax.random.normal(own_key, shape, jnp.float32)
    if shards:
        result = result * levels(own_key, shape, shards, -0.22, 0.18)
    return jnp.clip(result, -most, most).astype(kind)


def setup_inputs(seed: int = 0) -> dict:
    key_list = jax.random.split(jax.random.key(seed), 10)
    query = draw_query(jax.random.fold_in(key_list[9], 71), 0)
    keys = draw_keys(jax.random.fold_in(key_list[9], 71), 0)
    values = bell_draw(key_list[2], (IMAGES, PATCHES, D), 1.0, 6.0, ((0, 8), (1, 4)))
    out_weight = bell_draw(key_list[3], (D, D), D ** -0.5, 0.15625, ((0, 4),))
    hidden = draw_hidden(jax.random.fold_in(key_list[9], 71), 0)
    gain = jnp.clip(1.0 + 0.1 * jax.random.normal(key_list[5], (D,), jnp.float32), 0.5, 1.5)
    seq_grad = bell_draw(key_list[6], (IMAGES, SEQ_LEN, 4 * D), 1.0, 6.0, ((0, 8), (1, 4)))
    splice_at = draw_splice_at(jax.random.fold_in(key_list[9], 71), 0)
    merged_count = place_ends(jax.random.randint(key_list[8], (IMAGES,), MERGED // 8, MERGED + 1), jax.random.fold_in(key_list[8], 1), MERGED // 8, MERGED).astype(jnp.int32)
    return {"query": query, "keys": keys, "values": values, "out_weight": out_weight, "hidden": hidden, "gain": gain, "seq_grad": seq_grad, "splice_at": splice_at, "merged_count": merged_count}


norm_eps = 1e-06

def head_backward(packed, key_live):
    head_query, head_keys, head_values, head_grad = packed
    factor = HEAD ** (-0.5)
    scores = jnp.dot(head_query, head_keys.T, preferred_element_type=jnp.float32) * factor
    scores = jnp.where(key_live[None, :], scores, -1e+30)
    largest = lax.optimization_barrier(jnp.max(scores, axis=-1, keepdims=True))
    expons = jnp.exp(scores - largest)
    probs = expons / lax.optimization_barrier(jnp.sum(expons, axis=-1, keepdims=True))
    low_probs = probs.astype(jnp.bfloat16)
    value_part = jnp.dot(low_probs.T, head_grad, preferred_element_type=jnp.float32).astype(jnp.bfloat16)
    dprobs = jnp.dot(head_grad, head_values.T, preferred_element_type=jnp.float32)
    spread = lax.optimization_barrier(jnp.sum(probs * dprobs, axis=-1, keepdims=True))
    dscores = (probs * (dprobs - spread)).astype(jnp.bfloat16)
    query_part = (jnp.dot(dscores, head_keys, preferred_element_type=jnp.float32) * factor).astype(jnp.bfloat16)
    key_part = (jnp.dot(dscores.T, head_query, preferred_element_type=jnp.float32) * factor).astype(jnp.bfloat16)
    return (query_part, key_part, value_part)

def split_heads(matrix):
    return matrix.reshape(PATCHES, HEADS, HEAD).transpose(1, 0, 2)

def join_heads(stacked):
    return stacked.transpose(1, 0, 2).reshape(PATCHES, D)

def reference(query, keys, values, out_weight, hidden, gain, seq_grad, splice_at, merged_count):

    def image_grads(packed):
        query_img, keys_img, values_img, hidden_img, seq_img, spots_img, count_img = packed
        picked = jnp.take(seq_img, spots_img, axis=0)
        live_rows = jnp.arange(MERGED) < count_img
        merged = jnp.where(live_rows[:, None], picked, jnp.zeros((), picked.dtype))
        upstream = merged.reshape(PATCHES, D).astype(jnp.float32)
        values32 = hidden_img.astype(jnp.float32)
        inverse = lax.rsqrt(lax.optimization_barrier(jnp.mean(values32 * values32, axis=-1, keepdims=True)) + norm_eps)
        normed = values32 * inverse
        gain_part = lax.optimization_barrier(jnp.sum(upstream * normed, axis=0))
        scaled = gain * upstream
        attn_grad = (inverse * (scaled - normed * lax.optimization_barrier(jnp.mean(scaled * normed, axis=-1, keepdims=True)))).astype(jnp.bfloat16)
        core_grad = jnp.dot(attn_grad, out_weight.T, preferred_element_type=jnp.float32).astype(jnp.bfloat16)
        key_live = jnp.arange(PATCHES) < 4 * count_img
        stacked = lax.map(lambda item: head_backward(item, key_live), (split_heads(query_img), split_heads(keys_img), split_heads(values_img), split_heads(core_grad)))
        return (join_heads(stacked[0]), join_heads(stacked[1]), join_heads(stacked[2]), gain_part)
    query_grad, key_grad, value_grad, gain_parts = lax.map(image_grads, (query, keys, values, hidden, seq_grad, splice_at, merged_count))
    gain_grad = lax.optimization_barrier(jnp.sum(gain_parts, axis=0))
    return (query_grad, key_grad, value_grad, gain_grad)
```

```python
import functools

import jax
import jax.numpy as jnp
from jax import lax
from jax.experimental import pallas as pl
from jax.experimental.pallas import tpu as pltpu
from jax.sharding import PartitionSpec as P

HEAD = 80


norm_eps = 1e-06
low = jnp.bfloat16
full = jnp.float32


def splice_back(seq_grad, splice_at, merged_count, width):
    seq_rows = seq_grad[0]
    span_len = seq_rows.shape[0]
    tile_count = lax.axis_size("tile")
    my_tile = lax.axis_index("tile")
    positions = splice_at[0]
    rows_here = positions.shape[0]
    capacity = 2 * rows_here // tile_count
    owners = positions // span_len
    within = positions % span_len
    onehot = (owners[:, None] == jnp.arange(tile_count, dtype=jnp.int32)[None, :]).astype(jnp.int32)
    before = jnp.cumsum(onehot, axis=0) - onehot
    rank_in = jnp.sum(before * onehot, axis=1)
    slot_ids = owners * capacity + rank_in
    requests = jnp.full((tile_count * capacity,), -1, jnp.int32).at[slot_ids].set(within)
    requests = requests.reshape(tile_count, capacity)
    asked_for = lax.all_to_all(requests, "tile", split_axis=0, concat_axis=0, tiled=True)
    found_rows = jnp.take(seq_rows, jnp.clip(asked_for, 0, span_len - 1), axis=0)
    found_rows = jnp.where(
        (asked_for >= 0)[:, :, None], found_rows, jnp.zeros((), found_rows.dtype)
    )
    replies = lax.all_to_all(found_rows, "tile", split_axis=0, concat_axis=0, tiled=True)
    merged = replies.reshape(tile_count * capacity, -1)[slot_ids]
    live_rows = my_tile * rows_here + jnp.arange(rows_here) < merged_count[0]
    merged = jnp.where(live_rows[:, None], merged, jnp.zeros((), merged.dtype))
    return merged.reshape(-1, width)


def norm_backward(hidden, gain, patch_grad):
    values32 = hidden[0].astype(jnp.float32)
    inverse = lax.rsqrt(jnp.mean(values32 * values32, axis=-1, keepdims=True) + norm_eps)
    normed = values32 * inverse
    upstream = patch_grad.astype(jnp.float32)
    gain_part = jnp.sum(upstream * normed, axis=0)
    scaled = gain * upstream
    attn_grad = (
        inverse * (scaled - normed * jnp.mean(scaled * normed, axis=-1, keepdims=True))
    ).astype(jnp.bfloat16)
    return (attn_grad, gain_part)


def to_heads(matrix, tile_count):
    return matrix.reshape(matrix.shape[0], tile_count, -1)


def head_view(arrived):
    return arrived.reshape(arrived.shape[0], -1, HEAD)


def from_heads(result, tile_count, rows_here):
    return result.reshape(tile_count, rows_here, -1)


def attend(head_q, head_k, head_v, head_g, valid_keys):
    patches, heads_here, head_size = head_q.shape
    block = min(512, patches)
    factor = head_size ** (-0.5)
    key_live = jnp.arange(patches) < valid_keys

    def one_block(index, carried):
        grad_q, grad_k, grad_v = carried
        start = index * block
        query_block = lax.dynamic_slice_in_dim(head_q, start, block, 0)
        grads_block = lax.dynamic_slice_in_dim(head_g, start, block, 0)
        scores = (
            jnp.einsum("bhe,khe->hbk", query_block, head_k, preferred_element_type=jnp.float32)
            * factor
        )
        scores = jnp.where(key_live[None, None, :], scores, -1e30)
        largest = jnp.max(scores, axis=-1, keepdims=True)
        expons = jnp.exp(scores - largest)
        probs = expons / jnp.sum(expons, axis=-1, keepdims=True)
        low_probs = probs.astype(jnp.bfloat16)
        grad_v = grad_v + jnp.einsum(
            "hbk,bhe->khe", low_probs, grads_block, preferred_element_type=jnp.float32
        )
        dprobs = jnp.einsum("bhe,khe->hbk", grads_block, head_v, preferred_element_type=jnp.float32)
        spread = jnp.sum(probs * dprobs, axis=-1, keepdims=True)
        dscores = (probs * (dprobs - spread)).astype(jnp.bfloat16)
        block_grad = (
            jnp.einsum("hbk,khe->bhe", dscores, head_k, preferred_element_type=jnp.float32) * factor
        )
        grad_k = grad_k + jnp.einsum(
            "hbk,bhe->khe", dscores, query_block, preferred_element_type=jnp.float32
        )
        grad_q = lax.dynamic_update_slice_in_dim(grad_q, block_grad.astype(jnp.bfloat16), start, 0)
        return (grad_q, grad_k, grad_v)

    initial = (
        jnp.zeros(head_q.shape, jnp.bfloat16),
        jnp.zeros(head_q.shape, jnp.float32),
        jnp.zeros(head_q.shape, jnp.float32),
    )
    upper = patches // block
    grad_q, grad_k, grad_v = lax.fori_loop(0, upper, one_block, initial)
    return (grad_q, (grad_k * factor).astype(jnp.bfloat16), grad_v.astype(jnp.bfloat16))


def general_body(query, keys, values, out_weight, hidden, gain, seq_grad, splice_at, merged_count):
    tile_count = lax.axis_size("tile")
    width = query.shape[-1]
    rows_here = query.shape[1]
    head_q, head_k, head_v = (
        lax.all_to_all(to_heads(part[0], tile_count), "tile", split_axis=1, concat_axis=0, tiled=True)
        for part in (query, keys, values)
    )
    patch_grad = splice_back(seq_grad, splice_at, merged_count, width)
    attn_grad, gain_part = norm_backward(hidden, gain, patch_grad)
    head_g = jnp.einsum(
        "pd,cd->pc",
        lax.all_gather(attn_grad, "tile", axis=0, tiled=True),
        out_weight,
        preferred_element_type=jnp.float32,
    ).astype(jnp.bfloat16)
    gain_grad = lax.psum(gain_part, ("img", "tile"))
    valid_keys = 4 * merged_count[0]
    grads = attend(
        head_view(head_q), head_view(head_k), head_view(head_v), head_view(head_g), valid_keys
    )
    back_q, back_k, back_v = (
        lax.all_to_all(
            from_heads(part, tile_count, rows_here), "tile", split_axis=0, concat_axis=2, tiled=True
        )
        for part in grads
    )
    return (back_q, back_k, back_v, gain_grad)


NT = (((1,), (1,)), ((), ()))
NN = (((1,), (0,)), ((), ()))
TN = (((0,), (0,)), ((), ()))


def dot(left, right, form):
    return lax.dot_general(left, right, form, preferred_element_type=full)


def iota(shape, axis):
    return lax.broadcasted_iota(jnp.int32, shape, axis)


def ones_where(condition):
    return jnp.where(condition, 1.0, 0.0).astype(full)


def halves(width):
    pair = lax.div(lax.axis_index("tile"), 2)
    half = width // 2
    mine = pl.multiple_of(pair * half, 128)
    other = pl.multiple_of((1 - pair) * half, 128)
    return half, pl.ds(mine, half), pl.ds(other, half)


def run(kernel, name, outs, args, scalars=0, scratch=()):
    smem = pl.BlockSpec(memory_space=pltpu.SMEM)
    vmem = pl.BlockSpec(memory_space=pltpu.VMEM)
    return pl.pallas_call(
        kernel,
        name=name,
        out_shape=[jax.ShapeDtypeStruct(shape, kind) for shape, kind in outs],
        in_specs=[smem] * scalars + [vmem] * (len(args) - scalars),
        out_specs=[vmem] * len(outs),
        scratch_shapes=list(scratch),
        compiler_params=pltpu.CompilerParams(vmem_limit_bytes=48 * 1024 * 1024),
    )(*args)


def pack_kernel(q_ref, k_ref, v_ref, qs_ref, kvs_ref, kvo_ref):
    half, mine, other = halves(q_ref.shape[1])
    qs_ref[...] = q_ref[:, other]
    kvs_ref[:, :half] = k_ref[:, other]
    kvs_ref[:, half:] = v_ref[:, other]
    kvo_ref[:, :half] = k_ref[:, mine]
    kvo_ref[:, half:] = v_ref[:, mine]


def earlier(count):
    return ones_where(iota((count, count), 0) < iota((count, count), 1))


def reply_kernel(p0, p1, p2, p3, seq_ref, o0, o1, o2, o3):
    span, width = seq_ref.shape
    rows = p0.shape[1]
    cap = o0.shape[0]
    base = lax.axis_index("tile") * span
    before = earlier(rows)
    picks = []
    for place in (p0, p1, p2, p3):
        within = place[...] - base
        here = ones_where((within >= 0) & (within < span))
        rank = dot(jnp.broadcast_to(here, (8, rows)), before, NN)[:1]
        to_slot = ones_where(iota((cap, rows), 0).astype(full) == rank) * here
        to_place = ones_where(iota((span, rows), 0) == within)
        picks.append(dot(to_slot.astype(low), to_place.astype(low), NT))
    pick = jnp.concatenate(picks, axis=0).astype(low)
    step = width // 4
    for start in range(0, width, step):
        found = dot(pick, seq_ref[:, start : start + step], NN).astype(low)
        for x, out in enumerate((o0, o1, o2, o3)):
            out[:, start : start + step] = found[x * cap : (x + 1) * cap]


def norm_kernel(span, count_ref, place_ref, r0, r1, r2, r3, hidden_ref, gain_ref, attn_ref, part_ref, rows_buf, up_buf):
    me = lax.axis_index("tile")
    rows = place_ref.shape[1]
    cap = r0.shape[0]
    patches, width = hidden_ref.shape
    per = patches // rows
    for x, reply in enumerate((r0, r1, r2, r3)):
        rows_buf[x * cap : (x + 1) * cap] = reply[...]
    place = place_ref[...]
    here = jnp.zeros((8, rows), full)
    for x in range(4):
        within = place - jnp.bitwise_xor(me, x) * span
        inside = ones_where((within >= 0) & (within < span))
        here = here + ones_where(iota((8, rows), 0) == x) * inside
    rank = dot(here, earlier(rows), NN)
    slot = jnp.sum(here * (rank + cap * iota((8, rows), 0).astype(full)), axis=0, keepdims=True)
    from_slot = ones_where(iota((4 * cap, rows), 0).astype(full) == slot)
    live = ones_where(iota((1, rows), 1) + me * rows < count_ref[0])
    total = None
    for j in range(per):
        spread = ones_where(iota((patches, rows), 0) == per * iota((patches, rows), 1) + j) * live
        pick = dot(spread.astype(low), from_slot.astype(low), NT).astype(low)
        part = dot(pick, rows_buf[:, j * width : (j + 1) * width], NN)
        total = part if total is None else total + part
    up_buf[...] = total
    gain = gain_ref[...]
    step = 16
    kept = jnp.zeros((step, width), full)
    for start in range(0, patches, step):
        held = hidden_ref[start : start + step].astype(full)
        inverse = lax.rsqrt(jnp.mean(held * held, axis=-1, keepdims=True) + norm_eps)
        normed = held * inverse
        upstream = up_buf[start : start + step]
        kept = kept + upstream * normed
        scaled = gain * upstream
        mean = jnp.mean(scaled * normed, axis=-1, keepdims=True)
        attn_ref[start : start + step] = (inverse * (scaled - normed * mean)).astype(low)
    part_ref[...] = jnp.sum(kept, axis=0, keepdims=True)


def attend_kernel(
    count_ref, q_ref, q2_ref, kv0, kv1, kv2, kv3, a0, a2, w0, w1,
    dq0_ref, dq2_ref, send_ref, keep_ref,
    q_buf, k_buf, v_buf, g_buf, w_buf, bias_buf, dqt_buf, dk_buf, dv_buf,
):
    me = lax.axis_index("tile")
    core = lax.rem(me, 2)
    rows, width = q_ref.shape
    half, mine, other = halves(width)
    channels = w0.shape[0]
    w_buf[pl.ds(pl.multiple_of(core * channels, channels), channels)] = w0[...]
    w_buf[pl.ds(pl.multiple_of((1 - core) * channels, channels), channels)] = w1[...]
    q_buf[:rows] = q_ref[:, mine]
    q_buf[rows:] = q2_ref[...]
    valid = count_ref[0] * 4
    for x, part in enumerate((kv0, kv1, kv2, kv3)):
        block = slice(x * rows, (x + 1) * rows)
        k_buf[block] = part[:, :half]
        v_buf[block] = part[:, half:]
        index = jnp.bitwise_xor(me, x) * rows + iota((rows, 128), 0)
        bias_buf[block] = jnp.where(index < valid, 0.0, -1e30).astype(full)
    g_buf[:rows] = dot(a0[...], w_buf[...], NT).astype(low)
    g_buf[rows:] = dot(a2[...], w_buf[...], NT).astype(low)
    factor = HEAD ** (-0.5)
    for start in range(0, half, HEAD):
        columns = slice(start, start + HEAD)
        q = q_buf[:, columns]
        k = k_buf[:, columns]
        v = v_buf[:, columns]
        g = g_buf[:, columns]
        scores = dot(k, q, NT) * factor + bias_buf[:, :1]
        expons = jnp.exp(scores - jnp.max(scores, axis=0, keepdims=True))
        probs = expons * (1.0 / jnp.sum(expons, axis=0, keepdims=True))
        dv_buf[:, columns] = dot(probs.astype(low), g, NN)
        dprobs = dot(v, g, NT)
        spread = jnp.sum(probs * dprobs, axis=0, keepdims=True)
        dscores = (probs * (dprobs - spread)).astype(low)
        dk_buf[:, columns] = dot(dscores, q, NN) * factor
        dqt_buf[columns] = dot(k, dscores, TN) * factor
    dq = jnp.transpose(dqt_buf[...])
    dq0_ref[...] = dq[:rows].astype(low)
    dq2_ref[...] = dq[rows:].astype(low)
    for x in range(2):
        keep = slice(2 * x * rows, (2 * x + 1) * rows)
        send = slice((2 * x + 1) * rows, (2 * x + 2) * rows)
        out = slice(x * rows, (x + 1) * rows)
        keep_ref[out, :half] = dk_buf[keep]
        keep_ref[out, half:] = dv_buf[keep]
        send_ref[out, :half] = dk_buf[send]
        send_ref[out, half:] = dv_buf[send]


def add_kernel(keep_ref, came_ref, own_ref, back_ref):
    rows = own_ref.shape[0]
    own_ref[...] = (keep_ref[:rows] + came_ref[:rows]).astype(low)
    back_ref[...] = (keep_ref[rows:] + came_ref[rows:]).astype(low)


def join_kernel(dq0, dqr, own, back, q_out, k_out, v_out):
    half, mine, other = halves(q_out.shape[1])
    q_out[:, mine] = dq0[...]
    q_out[:, other] = dqr[...]
    k_out[:, mine] = own[:, :half]
    k_out[:, other] = back[:, :half]
    v_out[:, mine] = own[:, half:]
    v_out[:, other] = back[:, half:]


def swap(value, x, axis="tile"):
    return lax.ppermute(value, axis, [(i, i ^ x) for i in range(lax.axis_size(axis))])


def sum_everywhere(part):
    for axis in ("tile", "img"):
        x = 1
        while x < lax.axis_size(axis):
            part = part + swap(part, x, axis)
            x *= 2
    return part


def pairs_body(query, keys, values, out_weight, hidden, gain, seq_grad, splice_at, merged_count):
    rows, width = query.shape[1:]
    half = width // 2
    asked = splice_at.shape[1]
    span, seq_width = seq_grad.shape[1:]
    cap = asked // 2
    vmem = pltpu.VMEM

    place = [splice_at] + [swap(splice_at, x) for x in (1, 2, 3)]
    q_send, kv_send, kv0 = run(
        pack_kernel, "pack",
        [((rows, half), low), ((rows, width), low), ((rows, width), low)],
        (query[0], keys[0], values[0]),
    )
    kv2 = swap(kv_send, 2)
    q2 = swap(q_send, 2)
    kv1 = swap(kv0, 1)
    kv3 = swap(kv2, 1)
    weight1 = swap(out_weight, 1)

    found = run(reply_kernel, "reply", [((cap, seq_width), low)] * 4, (*place, seq_grad[0]))
    replies = [found[0]] + [swap(found[x], x) for x in (1, 2, 3)]
    attn0, gain_part = run(
        functools.partial(norm_kernel, span), "norm",
        [((rows, width), low), ((1, width), full)],
        (merged_count, splice_at, *replies, hidden[0], gain[None]),
        scalars=1,
        scratch=[vmem((4 * cap, seq_width), low), vmem((rows, width), full)],
    )
    attn2 = swap(attn0, 2)
    gain_grad = sum_everywhere(gain_part)[0]

    dq0, dq_send, send, keep = run(
        attend_kernel, "attend",
        [((rows, half), low), ((rows, half), low), ((2 * rows, width), full), ((2 * rows, width), full)],
        (merged_count, query[0], q2, kv0, kv1, kv2, kv3, attn0, attn2, out_weight, weight1),
        scalars=1,
        scratch=[
            vmem((2 * rows, half), low), vmem((4 * rows, half), low), vmem((4 * rows, half), low),
            vmem((2 * rows, half), low), vmem((half, width), low), vmem((4 * rows, 128), full),
            vmem((half, 2 * rows), full), vmem((4 * rows, half), full), vmem((4 * rows, half), full),
        ],
    )
    came = swap(send, 1)
    dq_back = swap(dq_send, 2)
    own, back_send = run(
        add_kernel, "add", [((rows, width), low)] * 2, (keep, came)
    )
    back = swap(back_send, 2)
    grads = run(join_kernel, "join", [((rows, width), low)] * 3, (dq0, dq_back, own, back))
    return (*(part[None] for part in grads), gain_grad)


def power_of_two(count):
    return count & (count - 1) == 0


def solution(mesh):
    paired = mesh.shape["tile"] == 4 and power_of_two(mesh.shape["img"])
    return jax.shard_map(
        pairs_body if paired else general_body,
        mesh=mesh,
        in_specs=(
            P("img", "tile", None),
            P("img", "tile", None),
            P("img", "tile", None),
            P("tile", None),
            P("img", "tile", None),
            P(),
            P("img", "tile", None),
            P("img", "tile"),
            P("img"),
        ),
        out_specs=(P("img", "tile", None), P("img", "tile", None), P("img", "tile", None), P()),
        check_vma=False,
    )
```

```python
import functools

import jax
import jax.numpy as jnp
from jax import lax
from jax.experimental import pallas as pl
from jax.experimental.pallas import tpu as pltpu
from jax.sharding import PartitionSpec as P


HEAD = 80


norm_eps = 1e-06
low = jnp.bfloat16
full = jnp.float32


def splice_back(seq_grad, splice_at, merged_count, width):
    seq_rows = seq_grad[0]
    span_len = seq_rows.shape[0]
    tile_count = lax.axis_size("tile")
    my_tile = lax.axis_index("tile")
    positions = splice_at[0]
    rows_here = positions.shape[0]
    capacity = 2 * rows_here // tile_count
    owners = positions // span_len
    within = positions % span_len
    onehot = (owners[:, None] == jnp.arange(tile_count, dtype=jnp.int32)[None, :]).astype(jnp.int32)
    before = jnp.cumsum(onehot, axis=0) - onehot
    rank_in = jnp.sum(before * onehot, axis=1)
    slot_ids = owners * capacity + rank_in
    requests = jnp.full((tile_count * capacity,), -1, jnp.int32).at[slot_ids].set(within)
    requests = requests.reshape(tile_count, capacity)
    asked_for = lax.all_to_all(requests, "tile", split_axis=0, concat_axis=0, tiled=True)
    found_rows = jnp.take(seq_rows, jnp.clip(asked_for, 0, span_len - 1), axis=0)
    found_rows = jnp.where(
        (asked_for >= 0)[:, :, None], found_rows, jnp.zeros((), found_rows.dtype)
    )
    replies = lax.all_to_all(found_rows, "tile", split_axis=0, concat_axis=0, tiled=True)
    merged = replies.reshape(tile_count * capacity, -1)[slot_ids]
    live_rows = my_tile * rows_here + jnp.arange(rows_here) < merged_count[0]
    merged = jnp.where(live_rows[:, None], merged, jnp.zeros((), merged.dtype))
    return merged.reshape(-1, width)


def norm_backward(hidden, gain, patch_grad):
    values32 = hidden[0].astype(jnp.float32)
    inverse = lax.rsqrt(jnp.mean(values32 * values32, axis=-1, keepdims=True) + norm_eps)
    normed = values32 * inverse
    upstream = patch_grad.astype(jnp.float32)
    gain_part = jnp.sum(upstream * normed, axis=0)
    scaled = gain * upstream
    attn_grad = (
        inverse * (scaled - normed * jnp.mean(scaled * normed, axis=-1, keepdims=True))
    ).astype(jnp.bfloat16)
    return (attn_grad, gain_part)


def to_heads(matrix, tile_count):
    return matrix.reshape(matrix.shape[0], tile_count, -1)


def head_view(arrived):
    return arrived.reshape(arrived.shape[0], -1, HEAD)


def from_heads(result, tile_count, rows_here):
    return result.reshape(tile_count, rows_here, -1)


def attend(head_q, head_k, head_v, head_g, valid_keys):
    patches, _, head_size = head_q.shape
    block = min(512, patches)
    factor = head_size ** (-0.5)
    key_live = jnp.arange(patches) < valid_keys

    def one_block(index, carried):
        grad_q, grad_k, grad_v = carried
        start = index * block
        query_block = lax.dynamic_slice_in_dim(head_q, start, block, 0)
        grads_block = lax.dynamic_slice_in_dim(head_g, start, block, 0)
        scores = (
            jnp.einsum("bhe,khe->hbk", query_block, head_k, preferred_element_type=jnp.float32)
            * factor
        )
        scores = jnp.where(key_live[None, None, :], scores, -1e30)
        largest = jnp.max(scores, axis=-1, keepdims=True)
        expons = jnp.exp(scores - largest)
        probs = expons / jnp.sum(expons, axis=-1, keepdims=True)
        low_probs = probs.astype(jnp.bfloat16)
        grad_v = grad_v + jnp.einsum(
            "hbk,bhe->khe", low_probs, grads_block, preferred_element_type=jnp.float32
        )
        dprobs = jnp.einsum("bhe,khe->hbk", grads_block, head_v, preferred_element_type=jnp.float32)
        spread = jnp.sum(probs * dprobs, axis=-1, keepdims=True)
        dscores = (probs * (dprobs - spread)).astype(jnp.bfloat16)
        block_grad = (
            jnp.einsum("hbk,khe->bhe", dscores, head_k, preferred_element_type=jnp.float32) * factor
        )
        grad_k = grad_k + jnp.einsum(
            "hbk,bhe->khe", dscores, query_block, preferred_element_type=jnp.float32
        )
        grad_q = lax.dynamic_update_slice_in_dim(grad_q, block_grad.astype(jnp.bfloat16), start, 0)
        return (grad_q, grad_k, grad_v)

    initial = (
        jnp.zeros(head_q.shape, jnp.bfloat16),
        jnp.zeros(head_q.shape, jnp.float32),
        jnp.zeros(head_q.shape, jnp.float32),
    )
    upper = patches // block
    grad_q, grad_k, grad_v = lax.fori_loop(0, upper, one_block, initial)
    return (grad_q, (grad_k * factor).astype(jnp.bfloat16), grad_v.astype(jnp.bfloat16))


def general_body(query, keys, values, out_weight, hidden, gain, seq_grad, splice_at, merged_count):
    tile_count = lax.axis_size("tile")
    width = query.shape[-1]
    rows_here = query.shape[1]
    head_q, head_k, head_v = (
        lax.all_to_all(to_heads(part[0], tile_count), "tile", split_axis=1, concat_axis=0, tiled=True)
        for part in (query, keys, values)
    )
    patch_grad = splice_back(seq_grad, splice_at, merged_count, width)
    attn_grad, gain_part = norm_backward(hidden, gain, patch_grad)
    head_g = jnp.einsum(
        "pd,cd->pc",
        lax.all_gather(attn_grad, "tile", axis=0, tiled=True),
        out_weight,
        preferred_element_type=jnp.float32,
    ).astype(jnp.bfloat16)
    gain_grad = lax.psum(gain_part, ("img", "tile"))
    valid_keys = 4 * merged_count[0]
    grads = attend(
        head_view(head_q), head_view(head_k), head_view(head_v), head_view(head_g), valid_keys
    )
    back_q, back_k, back_v = (
        lax.all_to_all(
            from_heads(part, tile_count, rows_here), "tile", split_axis=0, concat_axis=2, tiled=True
        )
        for part in grads
    )
    return (back_q, back_k, back_v, gain_grad)


NT = (((1,), (1,)), ((), ()))
NN = (((1,), (0,)), ((), ()))


def dot(left, right, form):
    return lax.dot_general(left, right, form, preferred_element_type=full)


def iota(shape, axis):
    return lax.broadcasted_iota(jnp.int32, shape, axis)


def ones_where(condition):
    return jnp.where(condition, 1.0, 0.0).astype(full)


def halves(width):
    pair = lax.div(lax.axis_index("tile"), 2)
    half = width // 2
    mine = pl.multiple_of(pair * half, 128)
    other = pl.multiple_of((1 - pair) * half, 128)
    return half, pl.ds(mine, half), pl.ds(other, half)


def run(kernel, outs, args, scalars=0, scratch=(), far=False, mebibytes=16, micros=2):
    smem = pl.BlockSpec(memory_space=pltpu.SMEM)
    vmem = pl.BlockSpec(memory_space=pltpu.VMEM)
    source = pl.BlockSpec(memory_space=pltpu.HBM) if far else vmem
    if far:
        args = [pltpu.with_memory_space_constraint(arg, pltpu.HBM) for arg in args]
    return pl.pallas_call(
        kernel,
        out_shape=[jax.ShapeDtypeStruct(shape, kind) for shape, kind in outs],
        in_specs=[smem] * scalars + [source] * (len(args) - scalars),
        out_specs=[vmem] * len(outs),
        scratch_shapes=list(scratch),
        compiler_params=pltpu.CompilerParams(vmem_limit_bytes=mebibytes * 2**20),
        cost_estimate=pl.CostEstimate(
            flops=micros * 10**6 * 8, bytes_accessed=micros * 10**6, transcendentals=0
        ),
    )(*args)


def copy_all(pairs, sems):
    copies = [pltpu.make_async_copy(a, b, sems.at[i]) for i, (a, b) in enumerate(pairs)]
    for copy in copies:
        copy.start()
    for copy in copies:
        copy.wait()


def pack_query_kernel(q_ref, q_send, sems):
    _, _, other = halves(q_ref.shape[1])
    step = q_ref.shape[0] // 4
    parts = [slice(i * step, (i + 1) * step) for i in range(4)]
    copy_all([(q_ref.at[part, other], q_send.at[part]) for part in parts], sems)


def pack_kernel(q_ref, k_ref, v_ref, q0, kv0, k_send, v_send, sems):
    half, mine, other = halves(q_ref.shape[1])
    copy_all(
        [
            (k_ref.at[:, other], k_send),
            (v_ref.at[:, other], v_send),
            (q_ref.at[:, mine], q0),
            (k_ref.at[:, mine], kv0.at[:, :half]),
            (v_ref.at[:, mine], kv0.at[:, half:]),
        ],
        sems,
    )


def load_kernel(seq_ref, out_ref, sems):
    step = seq_ref.shape[0] // 4
    copy_all(
        [
            (seq_ref.at[i * step : (i + 1) * step], out_ref.at[i * step : (i + 1) * step])
            for i in range(4)
        ],
        sems,
    )


def earlier(count):
    return ones_where(iota((count, count), 0) < iota((count, count), 1))


def reply_kernel(p0, p1, p2, p3, seq_ref, o0, o1, o2, o3):
    span, width = seq_ref.shape
    rows = p0.shape[1]
    cap = o0.shape[0]
    base = lax.axis_index("tile") * span
    before = earlier(rows)
    picks = []
    for place in (p0, p1, p2, p3):
        within = place[...] - base
        here = ones_where((within >= 0) & (within < span))
        rank = dot(jnp.broadcast_to(here, (8, rows)), before, NN)[:1]
        to_slot = ones_where(iota((cap, rows), 0).astype(full) == rank) * here
        to_place = ones_where(iota((span, rows), 0) == within)
        picks.append(dot(to_slot.astype(low), to_place.astype(low), NT))
    pick = jnp.concatenate(picks, axis=0).astype(low)
    step = width // 4
    for start in range(0, width, step):
        found = dot(pick, seq_ref[:, start : start + step], NN).astype(low)
        for x, out in enumerate((o0, o1, o2, o3)):
            out[:, start : start + step] = found[x * cap : (x + 1) * cap]


def norm_kernel(span, count_ref, place_ref, r0, r1, r2, r3, hidden_ref, gain_ref, attn_ref, part_ref, rows_buf, up_buf):
    me = lax.axis_index("tile")
    rows = place_ref.shape[1]
    cap = r0.shape[0]
    patches, width = hidden_ref.shape
    per = patches // rows
    for x, reply in enumerate((r0, r1, r2, r3)):
        rows_buf[x * cap : (x + 1) * cap] = reply[...]
    place = place_ref[...]
    here = jnp.zeros((8, rows), full)
    for x in range(4):
        within = place - jnp.bitwise_xor(me, x) * span
        inside = ones_where((within >= 0) & (within < span))
        here = here + ones_where(iota((8, rows), 0) == x) * inside
    rank = dot(here, earlier(rows), NN)
    slot = jnp.sum(here * (rank + cap * iota((8, rows), 0).astype(full)), axis=0, keepdims=True)
    from_slot = ones_where(iota((4 * cap, rows), 0).astype(full) == slot)
    live = ones_where(iota((1, rows), 1) + me * rows < count_ref[0])
    total = None
    for j in range(per):
        spread = ones_where(iota((patches, rows), 0) == per * iota((patches, rows), 1) + j) * live
        pick = dot(spread.astype(low), from_slot.astype(low), NT).astype(low)
        part = dot(pick, rows_buf[:, j * width : (j + 1) * width], NN)
        total = part if total is None else total + part
    up_buf[...] = total
    gain = gain_ref[...]
    step = 16
    kept = jnp.zeros((step, width), full)
    for start in range(0, patches, step):
        held = hidden_ref[start : start + step].astype(full)
        inverse = lax.rsqrt(jnp.mean(held * held, axis=-1, keepdims=True) + norm_eps)
        normed = held * inverse
        upstream = up_buf[start : start + step]
        kept = kept + upstream * normed
        scaled = gain * upstream
        mean = jnp.mean(scaled * normed, axis=-1, keepdims=True)
        attn_ref[start : start + step] = (inverse * (scaled - normed * mean)).astype(low)
    part_ref[...] = jnp.sum(kept, axis=0, keepdims=True)


def scores_kernel(
    count_ref, q0, q2, kv0, kv1, k2, k3, w0, w1,
    own_ref, far_ref, low_ref, qt_ref, kt_ref, w_ref, q_buf, k_buf, bias_buf,
):
    me = lax.axis_index("tile")
    core = lax.rem(me, 2)
    rows, half = q0.shape
    channels = w0.shape[0]
    w_ref[pl.ds(pl.multiple_of(core * channels, channels), channels)] = w0[...]
    w_ref[pl.ds(pl.multiple_of((1 - core) * channels, channels), channels)] = w1[...]
    q_buf[:rows] = q0[...]
    q_buf[rows:] = q2[...]
    valid = count_ref[0] * 4
    for x, part in enumerate((kv0, kv1, k2, k3)):
        block = slice(x * rows, (x + 1) * rows)
        k_buf[block] = part[:, :half]
        index = jnp.bitwise_xor(me, x) * rows + iota((rows, 128), 0)
        bias_buf[block] = jnp.where(index < valid, 0.0, -1e30).astype(full)
    patches = 4 * rows
    for head, start in enumerate(range(0, half, HEAD)):
        columns = slice(start, start + HEAD)
        scores = dot(k_buf[:, columns], q_buf[:, columns], NT) * HEAD ** (-0.5) + bias_buf[:, :1]
        expons = jnp.exp(scores - jnp.max(scores, axis=0, keepdims=True))
        probs = expons * (1.0 / jnp.sum(expons, axis=0, keepdims=True))
        block = slice(head * patches, (head + 1) * patches)
        own_ref[block] = probs[:, :rows]
        far_ref[block] = probs[:, rows:]
        low_ref[block] = probs.astype(low)
    qt_ref[...] = jnp.transpose(q_buf[...])
    kt_ref[...] = jnp.transpose(k_buf[...])


def half_grads(a_ref, w_ref, probs_ref, v_ref, kt_ref, gt_ref, ds_ref, dq_ref, turned):
    half = w_ref.shape[0]
    patches = kt_ref.shape[1]
    gt_ref[...] = dot(w_ref[...], a_ref[...], NT).astype(low)
    for head, start in enumerate(range(0, half, HEAD)):
        block = slice(head * patches, (head + 1) * patches)
        columns = slice(start, start + HEAD)
        probs = probs_ref[block]
        dprobs = dot(v_ref[block, :HEAD], gt_ref[columns], NN)
        spread = jnp.sum(probs * dprobs, axis=0, keepdims=True)
        ds_ref[block] = (probs * (dprobs - spread)).astype(low)
    for head, start in enumerate(range(0, half, HEAD)):
        columns = slice(start, start + HEAD)
        dscores = ds_ref[head * patches : (head + 1) * patches]
        turned[columns] = dot(kt_ref[columns], dscores, NN) * HEAD ** (-0.5)
    dq_ref[...] = jnp.transpose(turned[...]).astype(low)


def own_kernel(a_ref, w_ref, probs_ref, kv0, kv1, v2, v3, kt_ref, gt_ref, ds_ref, dq_ref, v_ref, turned):
    rows, half = v2.shape
    patches = 4 * rows
    for head, start in enumerate(range(0, half, HEAD)):
        for x, part in enumerate((kv0, kv1, v2, v3)):
            base = half + start if x < 2 else start
            block = slice(head * patches + x * rows, head * patches + (x + 1) * rows)
            v_ref[block, :HEAD] = part[:, base : base + HEAD]
    half_grads(a_ref, w_ref, probs_ref, v_ref, kt_ref, gt_ref, ds_ref, dq_ref, turned)


def keep_and_send(value, start, rows, keep_ref, send_ref):
    columns = slice(start, start + HEAD)
    for x in range(2):
        out = slice(x * rows, (x + 1) * rows)
        keep_ref[out, columns] = value[2 * x * rows : (2 * x + 1) * rows]
        send_ref[out, columns] = value[(2 * x + 1) * rows : (2 * x + 2) * rows]


def dv_kernel(probs_ref, g0_ref, g2_ref, keep_ref, send_ref):
    half, rows = g0_ref.shape
    patches = 4 * rows
    for head, start in enumerate(range(0, half, HEAD)):
        columns = slice(start, start + HEAD)
        grads = jnp.concatenate([g0_ref[columns], g2_ref[columns]], axis=1)
        dv = dot(probs_ref[head * patches : (head + 1) * patches], grads, NT)
        keep_and_send(dv, start, rows, keep_ref, send_ref)


def dk_kernel(ds0_ref, ds2_ref, qt_ref, keep_ref, send_ref):
    rows = ds0_ref.shape[1]
    half = qt_ref.shape[0]
    patches = 4 * rows
    for head, start in enumerate(range(0, half, HEAD)):
        block = slice(head * patches, (head + 1) * patches)
        dscores = jnp.concatenate([ds0_ref[block], ds2_ref[block]], axis=1)
        dk = dot(dscores, qt_ref[start : start + HEAD], NT) * HEAD ** (-0.5)
        keep_and_send(dk, start, rows, keep_ref, send_ref)


def add_kernel(keep_ref, came_ref, own_ref, back_ref):
    rows = own_ref.shape[0]
    own_ref[...] = (keep_ref[:rows] + came_ref[:rows]).astype(low)
    back_ref[...] = (keep_ref[rows:] + came_ref[rows:]).astype(low)


def join_kernel(own, back, out):
    _, mine, other = halves(out.shape[1])
    out[:, mine] = own[...]
    out[:, other] = back[...]


def last_join_kernel(part, came, own, back, out, gain_out):
    join_kernel(own, back, out)
    gain_out[...] = part[...] + came[...]


def swap(value, x, axis="tile"):
    return lax.ppermute(value, axis, [(i, i ^ x) for i in range(lax.axis_size(axis))])


def pairs_body(*args):
    return pairs_plan(*args)


def pairs_plan(query, keys, values, out_weight, hidden, gain, seq_grad, splice_at, merged_count):
    rows, width = query.shape[1:]
    half = width // 2
    heads = half // HEAD
    asked = splice_at.shape[1]
    span, seq_width = seq_grad.shape[1:]
    cap = asked // 2
    vmem, sems = pltpu.VMEM, pltpu.SemaphoreType.DMA
    block = ((rows, half), low)
    parts = ((2 * rows, half), full)

    place = [splice_at] + [swap(splice_at, x) for x in (1, 2, 3)]
    (q_send,) = run(pack_query_kernel, [block], (query[0],), far=True, scratch=[sems((4,))])
    q0, kv0, k_send, v_send = run(
        pack_kernel, [block, ((rows, width), low), block, block],
        (query[0], keys[0], values[0]), far=True, scratch=[sems((5,))],
    )
    q2 = swap(q_send, 2)
    k2 = swap(k_send, 2)
    v2 = swap(v_send, 2)
    kv1 = swap(kv0, 1)
    weight1 = swap(out_weight, 1)
    (seq_rows,) = run(
        load_kernel, [((span, seq_width), low)], (seq_grad[0],), far=True, scratch=[sems((4,))]
    )
    found = run(reply_kernel, [((cap, seq_width), low)] * 4, (*place, seq_rows))
    replies = [found[0]] + [swap(found[x], x) for x in (1, 2, 3)]
    k3 = swap(k2, 1)
    v3 = swap(v2, 1)
    stack = heads * 4 * rows
    turned = [vmem((half, rows), full)]
    probs0, probs2, probs, q_turned, k_turned, w_all = run(
        scores_kernel,
        [
            ((stack, rows), full), ((stack, rows), full), ((stack, 2 * rows), low),
            ((half, 2 * rows), low), ((half, 4 * rows), low), ((half, width), low),
        ],
        (merged_count, q0, q2, kv0, kv1, k2, k3, out_weight, weight1),
        scalars=1,
        scratch=[vmem((2 * rows, half), low), vmem((4 * rows, half), low), vmem((4 * rows, 128), full)],
    )
    attn0, gain_part = run(
        functools.partial(norm_kernel, span),
        [((rows, width), low), ((1, width), full)],
        (merged_count, splice_at, *replies, hidden[0], gain[None]),
        scalars=1, scratch=[vmem((4 * cap, seq_width), low), vmem((rows, width), full)],
    )
    attn2 = swap(attn0, 2)
    gain_came = swap(gain_part, 2)
    x = 1
    while x < lax.axis_size("img"):
        gain_part = gain_part + gain_came
        gain_came = swap(gain_part, x, "img")
        x = 2 * x
    gain_part = gain_part + gain_came
    gain_came = swap(gain_part, 1)

    half_outs = [((half, rows), low), ((stack, rows), low), block]
    grads0, dscores0, dq_own, v_heads = run(
        own_kernel, half_outs + [((stack, 128), low)],
        (attn0, w_all, probs0, kv0, kv1, v2, v3, k_turned), scratch=turned,
    )
    grads2, dscores2, dq_back = run(
        half_grads, half_outs, (attn2, w_all, probs2, v_heads, k_turned), scratch=turned
    )
    dq_far = swap(dq_back, 2)
    dv_keep, dv_send = run(dv_kernel, [parts, parts], (probs, grads0, grads2))
    dv_came = swap(dv_send, 1)
    dk_keep, dk_send = run(dk_kernel, [parts, parts], (dscores0, dscores2, q_turned))
    dk_came = swap(dk_send, 1)
    dv_own, dv_back = run(add_kernel, [block] * 2, (dv_keep, dv_came))
    dv_far = swap(dv_back, 2)
    dk_own, dk_back = run(add_kernel, [block] * 2, (dk_keep, dk_came))
    dk_far = swap(dk_back, 2)
    whole = [((rows, width), low)]
    (v_out,) = run(join_kernel, whole, (dv_own, dv_far))
    (q_out,) = run(join_kernel, whole, (dq_own, dq_far))
    k_out, gain_grad = run(
        last_join_kernel, whole + [((width,), full)],
        (gain_part[0], gain_came[0], dk_own, dk_far),
    )
    return (q_out[None], k_out[None], v_out[None], gain_grad)


def power_of_two(count):
    return count & (count - 1) == 0


def solution(mesh):
    paired = mesh.shape["tile"] == 4 and power_of_two(mesh.shape["img"])
    return jax.shard_map(
        pairs_body if paired else general_body,
        mesh=mesh,
        in_specs=(
            P("img", "tile", None),
            P("img", "tile", None),
            P("img", "tile", None),
            P("tile", None),
            P("img", "tile", None),
            P(),
            P("img", "tile", None),
            P("img", "tile"),
            P("img"),
        ),
        out_specs=(P("img", "tile", None), P("img", "tile", None), P("img", "tile", None), P()),
        check_vma=False,
    )
```
